32 devices in a mesh: dp: 32 (over z, y, x, core).
Axes of the slice: x: 2, y: 2, z: 4, core: 2. Of those that a mesh axis runs over, the one named last changes fastest.
Arguments:
- hidden: bfloat16 [32768, 5120], P('dp'), may hold values from -6 to 6
- norm_gain: float32 [5120], replicated, may hold values from 0.25 to 4
- q_cotangent: bfloat16 [32768, 128], P('dp'), may hold values from -0.03125 to 0.03125
- head_output: bfloat16 [32768, 128], P('dp'), may hold values from -6 to 6
- out_cotangent: bfloat16 [32768, 5120], P('dp'), may hold values from -0.0625 to 0.0625
- master_q: float32 [5120, 128], P('dp'), may hold values from -0.125 to 0.125
- moment_q: float32 [5120, 128], P('dp'), may hold values from -6 to 6
- second_q: float32 [5120, 128], P('dp'), may hold values from 0.01 to 0.5
- master_o: float32 [128, 5120], P(None, 'dp'), may hold values from -0.0234375 to 0.0234375
- moment_o: float32 [128, 5120], P(None, 'dp'), may hold values from -6 to 6
- second_o: float32 [128, 5120], P(None, 'dp'), may hold values from 0.01 to 0.5
Outputs:
- q_param: bfloat16 [5120, 128], replicated
- o_param: bfloat16 [128, 5120], replicated
- master_q_new: float32 [5120, 128], P('dp')
- moment_q_new: float32 [5120, 128], P('dp')
- second_q_new: float32 [5120, 128], P('dp')
- master_o_new: float32 [128, 5120], P(None, 'dp')
- moment_o_new: float32 [128, 5120], P(None, 'dp')
- second_o_new: float32 [128, 5120], P(None, 'dp')
- grad_rms: float32 [], replicated
The draws below stay inside these ranges and needn't reach their ends.
All inputs are finite; a program needn't handle non-finite values.
Results may differ from the reference program's by a relative error of at most 0.0026.
Values may be sent and summed in bfloat16 or wider, within the bound.
A program may use at most 128 MiB of HBM per device.

```python
import math
import jax
import jax.numpy as jnp
from jax import lax

D = 5120
WIDTH = 128
STEP = 20
TOK_DEV = 1024
TOKENS = 32768
N_DP = 32


def strengthened(drawn, rng, source, target, parts, factor):
    owner, partner = [(jnp.arange(drawn.shape[axis_at]) // (drawn.shape[axis_at] // parts)).reshape([-1 if axis == axis_at else 1 for axis in range(drawn.ndim)]) for axis_at in (source, target)]
    chosen = jax.random.permutation(rng, parts)[partner]
    strong = (owner == chosen) | (owner == (partner + parts // 2) % parts)
    return jnp.where(strong, factor * drawn, drawn)


def block_levels(own_key, shape, cuts, low, high):
    gain = 1.0
    for axis_at, shards_of in cuts:
        heights = jax.random.uniform(jax.random.fold_in(jax.random.fold_in(own_key, 6), axis_at), (shards_of,), jnp.float32, low / len(cuts), high / len(cuts))
        gain = gain * jnp.repeat(jnp.exp(heights), shape[axis_at] // shards_of).reshape((-1,) + (1,) * (len(shape) - 1 - axis_at))
    return gain


def gaussian(own_key, shape, width, reach, shards=(), held_as=jnp.bfloat16):
    drawn = jax.random.normal(own_key, shape, jnp.float32) * width
    if len(shards) > 0:
        drawn = block_levels(own_key, shape, shards, -0.22, 0.18) * drawn
    return jnp.clip(drawn, min=-reach, max=reach).astype(held_as)


def heavy_noise(key, dims, spread, bound, shards, heavy, held_as=jnp.bfloat16):
    array = spread * jax.random.normal(key, dims, jnp.float32)
    if shards:
        array = array * block_levels(key, dims, shards, -0.22, 0.18)
    return jnp.clip(strengthened(array, jax.random.fold_in(key, 3), *heavy), -bound, bound).astype(held_as)


def setup_inputs(seed: int = 0) -> dict:
    streams_of = jax.random.split(jax.random.key(seed), 12)
    hidden = heavy_noise(streams_of[0], (TOKENS, D), 1.0, 6.0, ((0, 32),), (0, 1, 32, 2.75))
    norm_gain = jnp.clip(jnp.exp(jax.random.uniform(streams_of[1], (D,), jnp.float32, math.log(0.25), math.log(4.0))), 0.25, 4.0)
    q_cotangent = gaussian(streams_of[2], (TOKENS, WIDTH), TOKENS ** -0.5, 0.03125, ((0, 32),))
    head_output = gaussian(streams_of[3], (TOKENS, WIDTH), 1.0, 6.0, ((0, 32),))
    out_cotangent = heavy_noise(streams_of[4], (TOKENS, D), TOKENS ** -0.5, 0.0625, ((0, 32),), (0, 1, 32, 2.75))
    master_q = gaussian(streams_of[5], (D, WIDTH), 0.009, 0.125, ((0, 32),), jnp.float32)
    moment_q = gaussian(streams_of[6], (D, WIDTH), 0.5, 6.0, ((0, 32),), jnp.float32)
    second_q = jnp.clip(jnp.exp(math.log(0.5) - 3.912023 * jax.random.uniform(streams_of[7], (D, WIDTH), jnp.float32) ** block_levels(streams_of[7], (D, WIDTH), ((0, 32),), -0.2, 0.2)), 0.01, 0.5)
    master_o = gaussian(streams_of[8], (WIDTH, D), 0.0015, 0.0234375, ((1, 32),), jnp.float32)
    moment_o = gaussian(streams_of[9], (WIDTH, D), 0.5, 6.0, ((1, 32),), jnp.float32)
    second_o = jnp.clip(jnp.exp(math.log(0.5) - 3.912023 * jax.random.uniform(streams_of[10], (WIDTH, D), jnp.float32) ** block_levels(streams_of[10], (WIDTH, D), ((1, 32),), -0.2, 0.2)), 0.01, 0.5)
    return dict(hidden=hidden, norm_gain=norm_gain, q_cotangent=q_cotangent, head_output=head_output, out_cotangent=out_cotangent, master_q=master_q, moment_q=moment_q, second_q=second_q, master_o=master_o, moment_o=moment_o, second_o=second_o)


norm_eps = 1e-05
beta_one = 0.9
beta_two = 0.95
learn_rate = 0.001
decay_rate = 0.1
adam_eps = 1e-08
clip_rms = 1.0

def normalize(hidden_block, norm_gain):
    hidden_wide = hidden_block.astype(jnp.float32)
    inverse = lax.rsqrt(lax.optimization_barrier(jnp.mean(hidden_wide * hidden_wide, axis=1, keepdims=True)) + norm_eps)
    return (hidden_wide * inverse * norm_gain[None, :]).astype(jnp.bfloat16)

def adamw(master, moment, second, gradient, factor):
    clipped = gradient * factor
    moment_new = beta_one * moment + (1.0 - beta_one) * clipped
    second_new = beta_two * second + (1.0 - beta_two) * clipped * clipped
    first_fix = 1.0 - beta_one ** STEP
    second_fix = 1.0 - beta_two ** STEP
    update = moment_new / first_fix / (jnp.sqrt(second_new / second_fix) + adam_eps)
    master_new = master - learn_rate * (update + decay_rate * master)
    return (master_new, moment_new, second_new)

def reference(hidden, norm_gain, q_cotangent, head_output, out_cotangent, master_q, moment_q, second_q, master_o, moment_o, second_o):

    def accumulate(carry, index):
        first_row = index * TOK_DEV
        hidden_block = lax.dynamic_slice_in_dim(hidden, first_row, TOK_DEV, 0)
        query_block = lax.dynamic_slice_in_dim(q_cotangent, first_row, TOK_DEV, 0)
        head_block = lax.dynamic_slice_in_dim(head_output, first_row, TOK_DEV, 0)
        outer_block = lax.dynamic_slice_in_dim(out_cotangent, first_row, TOK_DEV, 0)
        normed = normalize(hidden_block, norm_gain)
        grad_query = carry[0] + jnp.dot(normed.T, query_block, preferred_element_type=jnp.float32)
        grad_outer = carry[1] + jnp.dot(head_block.T, outer_block, preferred_element_type=jnp.float32)
        return ((grad_query, grad_outer), None)
    initial = (jnp.zeros((D, WIDTH), jnp.float32), jnp.zeros((WIDTH, D), jnp.float32))
    totals, unused = lax.scan(accumulate, initial, jnp.arange(N_DP, dtype=jnp.int32))
    grad_query, grad_outer = totals
    total_square = jnp.sum(grad_query * grad_query) + jnp.sum(grad_outer * grad_outer)
    grad_rms = jnp.sqrt(total_square / (2.0 * D * WIDTH))
    factor = jnp.minimum(1.0, clip_rms / grad_rms)
    master_q_new, moment_q_new, second_q_new = adamw(master_q, moment_q, second_q, grad_query, factor)
    master_o_new, moment_o_new, second_o_new = adamw(master_o, moment_o, second_o, grad_outer, factor)
    q_param = master_q_new.astype(jnp.bfloat16)
    o_param = master_o_new.astype(jnp.bfloat16)
    return (q_param, o_param, master_q_new, moment_q_new, second_q_new, master_o_new, moment_o_new, second_o_new, grad_rms)
```

```python
import functools
import math

import jax
import jax.numpy as jnp
from jax import lax
from jax.experimental import pallas as pl
from jax.experimental.pallas import tpu as pltpu
from jax.sharding import PartitionSpec as P

STEP = 20
norm_eps = 1e-05
beta_one = 0.9
beta_two = 0.95
learn_rate = 0.001
decay_rate = 0.1
adam_eps = 1e-08
clip_rms = 1.0
MESH = pl.DeviceIdType.MESH
F32 = jnp.float32
BF16 = jnp.bfloat16


def adamw(master, moment, second, gradient, factor):
    clipped = gradient * factor
    moment_new = beta_one * moment + (1.0 - beta_one) * clipped
    second_new = beta_two * second + (1.0 - beta_two) * clipped * clipped
    first_fix = 1.0 - beta_one**STEP
    second_fix = 1.0 - beta_two**STEP
    update = moment_new / first_fix / (jnp.sqrt(second_new / second_fix) + adam_eps)
    master_new = master - learn_rate * (update + decay_rate * master)
    return (master_new, moment_new, second_new)


def kernel(
    n, s, zs,
    hid_ref, gain_ref, qt_ref, ht_ref, oc_ref, st_ref,
    gbuf, new_ref, rms_ref,
    hid, oc, inv, part, crecv, asend, arecv, bsend, brecv, zsend, zrecv, sbuf,
    hsem, osem, c_s, c_r, a_s, a_r, b_s, b_r, z_s, z_r, s_s, s_r,
    gz_s, gz_r, gb_s, gb_r, ga_s, ga_r, gc_s, gc_r,
):
    tokens, width = hid.shape
    rows = part.shape[2]
    me = lax.axis_index("dp")
    core = me % 2
    x = (me // 2) % s
    y = (me // (2 * s)) % s
    z = me // (2 * s * s)
    a = x + core * (y - x)
    b = y + core * (x - y)
    other = 1 - core

    def dev(c, a_at, b_at, z_at):
        x_at = a_at + c * (b_at - a_at)
        y_at = b_at + c * (a_at - b_at)
        return ((z_at * s + y_at) * s + x_at) * 2 + c

    def remote(src, dst, ss, rs, to):
        return pltpu.make_async_remote_copy(
            src_ref=src, dst_ref=dst, send_sem=ss, recv_sem=rs, device_id=(to,), device_id_type=MESH
        )

    chunk = rows * 128 // math.gcd(rows, 128)
    chunk = chunk * max(1, 640 // chunk)
    steps = width // chunk
    per = chunk // rows
    hrow = tokens // 4

    oc_in = [
        pltpu.make_async_copy(oc_ref.at[:, pl.ds(i * chunk, chunk)], oc.at[:, pl.ds(i * chunk, chunk)], osem.at[i])
        for i in range(steps)
    ]
    hid_in = [
        pltpu.make_async_copy(hid_ref.at[pl.ds(i * hrow, hrow)], hid.at[pl.ds(i * hrow, hrow)], hsem.at[i])
        for i in range(4)
    ]
    for copy in oc_in + hid_in:
        copy.start()

    peer_c = dev(other, b, a, z)
    peer_a = {d: dev(core, (a + d) % s, b, z) for d in range(1, s)}
    peer_b = {d: dev(core, a, (b + d) % s, z) for d in range(1, s)}
    peer_z = {d: dev(core, a, b, (z + d) % zs) for d in range(1, zs)}
    peers = [peer_c] + list(peer_a.values()) + list(peer_b.values()) + list(peer_z.values())
    barrier = pltpu.get_barrier_semaphore()
    for peer in peers:
        pl.semaphore_signal(barrier, inc=1, device_id=(peer,), device_id_type=MESH)
    pl.semaphore_wait(barrier, len(peers))

    sends = []

    def go(copy):
        copy.start()
        sends.append(copy)

    def send_chunk(h, i):
        for k in range(per // 2):
            j = i * per + 2 * k + other
            xj = (j // 2) % s
            yj = (j // (2 * s)) % s
            zj = j // (2 * s * s)
            aj = xj + other * (yj - xj)
            bj = yj + other * (xj - yj)
            d = (aj - b + s) % s
            e = (bj - a + s) % s
            f = (zj - z + zs) % zs
            slot = (d * s + e) * zs + f
            go(remote(part.at[h, j], crecv.at[h, slot], c_s.at[h, slot], c_r.at[h, slot], peer_c))

    def wait_c(h, d, e, f):
        slot = (d * s + e) * zs + f
        remote(part.at[h, 0], crecv.at[h, slot], c_s.at[h, slot], c_r.at[h, slot], peer_c).wait_recv()

    def pair(h, d, e, f):
        j = dev(core, (a + d) % s, (b + e) % s, (z + f) % zs)
        return part[h, j] + crecv[h, (d * s + e) * zs + f]

    e_order = list(range(1, s)) + [0]
    f_order = [f for f in (2, 1, 3) if f < zs] + [0]

    def copy_a(h, d, e, f):
        at = ((d - 1) * s + e) * zs + f
        return remote(asend.at[h, at], arecv.at[h, at], a_s.at[h, at], a_r.at[h, at], peer_a[d])

    def copy_b(h, e, f):
        at = (e - 1) * zs + f
        return remote(bsend.at[h, at], brecv.at[h, at], b_s.at[h, at], b_r.at[h, at], peer_b[e])

    def copy_z(h, f):
        return remote(zsend.at[h, f - 1], zrecv.at[h, f - 1], z_s.at[h, f - 1], z_r.at[h, f - 1], peer_z[f])

    def stage_a(h):
        for e in e_order:
            for f in f_order:
                for d in range(1, s):
                    wait_c(h, d, e, f)
                    asend[h, ((d - 1) * s + e) * zs + f] = pair(h, d, e, f).astype(BF16)
                    go(copy_a(h, d, e, f))

    def after_a(h, e, f):
        wait_c(h, 0, e, f)
        total = pair(h, 0, e, f)
        for d in range(1, s):
            copy_a(h, d, e, f).wait_recv()
            total += arecv[h, ((d - 1) * s + e) * zs + f].astype(F32)
        return total

    def stage_b(h):
        for f in f_order:
            for e in range(1, s):
                bsend[h, (e - 1) * zs + f] = after_a(h, e, f).astype(BF16)
                go(copy_b(h, e, f))

    def after_b(h, f):
        total = after_a(h, 0, f)
        for e in range(1, s):
            copy_b(h, e, f).wait_recv()
            total += brecv[h, (e - 1) * zs + f].astype(F32)
        return total

    def stage_z(h):
        for f in f_order[:-1]:
            zsend[h, f - 1] = after_b(h, f).astype(BF16)
            go(copy_z(h, f))

    def finish(h):
        total = after_b(h, 0)
        for f in range(1, zs):
            copy_z(h, f).wait_recv()
            total += zrecv[h, f - 1].astype(F32)
        return total

    def store(h, i, product):
        turned = product.T
        for k in range(per):
            part[h, i * per + k] = turned[k * rows : (k + 1) * rows]

    head = ht_ref[...]
    for i in range(steps):
        oc_in[i].wait()
        store(0, i, jnp.dot(head, oc[:, i * chunk : (i + 1) * chunk], preferred_element_type=F32))
        send_chunk(0, i)

    group = 16
    for i in range(4):
        hid_in[i].wait()

        @pl.loop(0, hrow // group)
        def squares(t, i=i):
            at = pl.multiple_of(i * hrow + t * group, group)
            wide = hid[pl.ds(at, group)].astype(F32)
            inv[pl.ds(at, group)] = lax.rsqrt(jnp.sum(wide * wide, axis=1, keepdims=True) / width + norm_eps)

    stage_a(0)

    scaled = qt_ref[...].astype(F32) * inv[...]
    high = scaled.astype(BF16)
    low = (scaled - high.astype(F32)).astype(BF16)
    both = jnp.concatenate([high, low], axis=1).T
    cols = qt_ref.shape[1]
    for i in range(steps):
        product = jnp.dot(both, hid[:, i * chunk : (i + 1) * chunk], preferred_element_type=F32)
        store(1, i, (product[:cols] + product[cols:]) * gain_ref[:, i * chunk : (i + 1) * chunk])
        send_chunk(1, i)

    stage_b(0)
    stage_a(1)
    stage_z(0)
    stage_b(1)
    stage_z(1)
    grad_o = finish(0)
    part[0, me] = grad_o
    grad_q = finish(1)
    part[1, me] = grad_q

    square = jnp.sum(grad_q * grad_q) + jnp.sum(grad_o * grad_o)
    value = jnp.full(sbuf.shape[2:], square, F32)
    at_sem = 0
    for stage, (place, size, to) in enumerate(
        ((core, 2, {1: peer_c}), (a, s, peer_a), (b, s, peer_b), (z, zs, peer_z))
    ):
        sbuf[stage, place] = value
        copies = []
        for d in range(1, size):
            copy = remote(sbuf.at[stage, place], sbuf.at[stage, place], s_s.at[at_sem], s_r.at[at_sem], to[d])
            at_sem += 1
            go(copy)
            copies.append((d, copy))
        for d, copy in copies:
            copy.wait_recv()
        value = sbuf[stage, 0]
        for k in range(1, size):
            value = value + sbuf[stage, k]
    rms = jnp.sqrt(value / (2.0 * width * cols))
    rms_ref[...] = rms
    factor = jnp.minimum(1.0, clip_rms / rms)[:1]

    for h in (1, 0):
        master, moment, second = adamw(st_ref[3 * h], st_ref[3 * h + 1], st_ref[3 * h + 2], part[h, me], factor)
        new_ref[3 * h] = master
        new_ref[3 * h + 1] = moment
        new_ref[3 * h + 2] = second
        gbuf[me, h] = master.astype(BF16)

    def shard(d, e, f):
        return gbuf.at[dev(core, (a - d + s) % s, (b - e + s) % s, (z - f + zs) % zs)]

    def gather_z(f):
        return remote(shard(0, 0, 0), shard(0, 0, 0), gz_s.at[f - 1], gz_r.at[f - 1], peer_z[f])

    def gather_b(e, f):
        at = (e - 1) * zs + f
        return remote(shard(0, 0, f), shard(0, 0, f), gb_s.at[at], gb_r.at[at], peer_b[e])

    def gather_a(d, e, f):
        at = ((d - 1) * s + e) * zs + f
        return remote(shard(0, e, f), shard(0, e, f), ga_s.at[at], ga_r.at[at], peer_a[d])

    def gather_c(d, e, f):
        at = (d * s + e) * zs + f
        return remote(shard(d, e, f), shard(d, e, f), gc_s.at[at], gc_r.at[at], peer_c)

    def pass_a(e, f):
        for d in range(1, s):
            go(gather_a(d, e, f))
        go(gather_c(0, e, f))

    def pass_b(f):
        if f:
            gather_z(f).wait_recv()
        for e in range(1, s):
            go(gather_b(e, f))
        pass_a(0, f)

    def from_b(f):
        for e in range(1, s):
            gather_b(e, f).wait_recv()
            pass_a(e, f)

    def from_a(f):
        for e in range(s):
            for d in range(1, s):
                gather_a(d, e, f).wait_recv()
                go(gather_c(d, e, f))

    for f in range(1, zs):
        go(gather_z(f))
    order = [0] + [f for f in (1, 3, 2) if f < zs]
    for t, f in enumerate(order):
        pass_b(f)
        from_b(f)
        if t:
            from_a(order[t - 1])
    from_a(order[-1])
    for d in range(s):
        for e in range(s):
            for f in range(zs):
                gather_c(d, e, f).wait_recv()
    for copy in sends:
        copy.wait_send()


def shards(
    hidden, norm_gain, q_cotangent, head_output, out_cotangent,
    master_q, moment_q, second_q, master_o, moment_o, second_o,
    *, n,
):
    tokens, width = hidden.shape
    rows, cols = master_q.shape
    zs = 4
    s = math.isqrt(n // (2 * zs))
    slots = s * s * zs
    state = jnp.stack([master_o.T, moment_o.T, second_o.T, master_q, moment_q, second_q])
    any_spec = pl.BlockSpec(memory_space=pl.ANY)
    vmem = pl.BlockSpec(memory_space=pltpu.VMEM)
    dma = pltpu.SemaphoreType.DMA
    na, nb, nz = (s - 1) * s * zs, (s - 1) * zs, zs - 1
    tile = (rows, cols)
    gathered, new, rms = pl.pallas_call(
        functools.partial(kernel, n, s, zs),
        out_shape=(
            jax.ShapeDtypeStruct((n, 2) + tile, BF16),
            jax.ShapeDtypeStruct((6,) + tile, F32),
            jax.ShapeDtypeStruct((8, 128), F32),
        ),
        in_specs=[any_spec, vmem, vmem, vmem, any_spec, vmem],
        out_specs=(vmem, vmem, vmem),
        scratch_shapes=[
            pltpu.VMEM((tokens, width), BF16),
            pltpu.VMEM((tokens, width), BF16),
            pltpu.VMEM((tokens, 1), F32),
            pltpu.VMEM((2, n) + tile, F32),
            pltpu.VMEM((2, slots) + tile, F32),
            pltpu.VMEM((2, na) + tile, BF16),
            pltpu.VMEM((2, na) + tile, BF16),
            pltpu.VMEM((2, nb) + tile, BF16),
            pltpu.VMEM((2, nb) + tile, BF16),
            pltpu.VMEM((2, nz) + tile, BF16),
            pltpu.VMEM((2, nz) + tile, BF16),
            pltpu.VMEM((4, max(s, zs), 8, 128), F32),
            dma((4,)), dma((64,)),
            dma((2, slots)), dma((2, slots)),
            dma((2, na)), dma((2, na)),
            dma((2, nb)), dma((2, nb)),
            dma((2, nz)), dma((2, nz)),
            dma((2 * s + zs,)), dma((2 * s + zs,)),
            dma((nz,)), dma((nz,)),
            dma((nb,)), dma((nb,)),
            dma((na,)), dma((na,)),
            dma((slots,)), dma((slots,)),
        ],
        compiler_params=pltpu.CompilerParams(
            collective_id=0, has_side_effects=True, vmem_limit_bytes=60 * 1024 * 1024
        ),
    )(hidden, norm_gain[None, :], q_cotangent, head_output.T, out_cotangent, state)
    q_param = gathered[:, 1].reshape(width, cols)
    o_param = gathered[:, 0].reshape(width, cols).T
    return (
        q_param, o_param,
        new[3], new[4], new[5],
        new[0].T, new[1].T, new[2].T,
        rms[0, 0],
    )


def solution(mesh):
    row, col = P("dp", None), P(None, "dp")
    in_specs = (row, P(), row, row, row, row, row, row, col, col, col)
    out_specs = (P(), P(), row, row, row, col, col, col, P())
    body = functools.partial(shards, n=mesh.shape["dp"])
    return jax.shard_map(body, mesh=mesh, in_specs=in_specs, out_specs=out_specs, check_vma=False)
```

```python
import functools
import math

import jax
import jax.numpy as jnp
from jax import lax
from jax.experimental import pallas as pl
from jax.experimental.pallas import tpu as pltpu
from jax.sharding import PartitionSpec as P

STEP = 20
norm_eps = 1e-05
beta_one = 0.9
beta_two = 0.95
learn_rate = 0.001
decay_rate = 0.1
adam_eps = 1e-08
clip_rms = 1.0
MESH = pl.DeviceIdType.MESH
F32 = jnp.float32
BF16 = jnp.bfloat16


def adamw(master, moment, second, gradient, factor):
    clipped = gradient * factor
    moment_new = beta_one * moment + (1.0 - beta_one) * clipped
    second_new = beta_two * second + (1.0 - beta_two) * clipped * clipped
    first_fix = 1.0 - beta_one**STEP
    second_fix = 1.0 - beta_two**STEP
    update = moment_new / first_fix / (jnp.sqrt(second_new / second_fix) + adam_eps)
    master_new = master - learn_rate * (update + decay_rate * master)
    return (master_new, moment_new, second_new)


def kernel(
    n, s, zs,
    hid_ref, gain_ref, qt_ref, ht_ref, oc_ref, st0, st1, st2, st3, st4, st5,
    gbuf_o, gbuf_q, new_ref, rms_ref,
    st_ref, hid, oc, inv, part, crecv, asend, arecv, bsend, brecv, zsend, zrecv, sbuf, tbuf,
    tsem, hsem, osem, c_s, c_r, a_s, a_r, b_s, b_r, z_s, z_r, s_s, s_r,
    gz_s, gz_r, gb_s, gb_r, ga_s, ga_r, gc_s, gc_r,
):
    tokens, width = hid.shape
    rows = part.shape[2]
    me = lax.axis_index("dp")
    core = me % 2
    x = (me // 2) % s
    y = (me // (2 * s)) % s
    z = me // (2 * s * s)
    a = x + core * (y - x)
    b = y + core * (x - y)
    other = 1 - core

    def dev(c, a_at, b_at, z_at):
        x_at = a_at + c * (b_at - a_at)
        y_at = b_at + c * (a_at - b_at)
        return ((z_at * s + y_at) * s + x_at) * 2 + c

    def remote(src, dst, ss, rs, to):
        return pltpu.make_async_remote_copy(
            src_ref=src, dst_ref=dst, send_sem=ss, recv_sem=rs, device_id=(to,), device_id_type=MESH
        )

    chunk = rows * 128 // math.gcd(rows, 128)
    chunk = chunk * max(1, 640 // chunk)
    steps = width // chunk
    per = chunk // rows
    hrow = tokens // 4

    oc_in = [
        pltpu.make_async_copy(oc_ref.at[:, pl.ds(i * chunk, chunk)], oc.at[:, pl.ds(i * chunk, chunk)], osem.at[i])
        for i in range(steps)
    ]
    hid_in = [
        pltpu.make_async_copy(hid_ref.at[pl.ds(i * hrow, hrow)], hid.at[pl.ds(i * hrow, hrow)], hsem.at[i])
        for i in range(4)
    ]
    states = [pltpu.make_async_copy(ref, st_ref.at[i], tsem.at[i]) for i, ref in enumerate((st0, st1, st2, st3, st4, st5))]
    for copy in oc_in + hid_in + states:
        copy.start()
    gbuf = (gbuf_o, gbuf_q)
    plane = 2 * s * s
    spot = me % plane

    peer_c = dev(other, b, a, z)
    peer_a = {d: dev(core, (a + d) % s, b, z) for d in range(1, s)}
    peer_b = {d: dev(core, a, (b + d) % s, z) for d in range(1, s)}
    peer_z = {d: dev(core, a, b, (z + d) % zs) for d in range(1, zs)}
    peer_p = {d: z * plane + (spot + d) % plane for d in range(1, plane)}
    peers = list(peer_p.values()) + list(peer_z.values())
    barrier = pltpu.get_barrier_semaphore()
    for peer in peers:
        pl.semaphore_signal(barrier, inc=1, device_id=(peer,), device_id_type=MESH)
    pl.semaphore_wait(barrier, len(peers))

    sends = []

    def go(copy):
        copy.start()
        sends.append(copy)

    def send_chunk(h, i):
        for k in range(per // 2):
            j = i * per + 2 * k + other
            xj = (j // 2) % s
            yj = (j // (2 * s)) % s
            zj = j // (2 * s * s)
            aj = xj + other * (yj - xj)
            bj = yj + other * (xj - yj)
            d = (aj - b + s) % s
            e = (bj - a + s) % s
            f = (zj - z + zs) % zs
            slot = (d * s + e) * zs + f
            go(remote(part.at[h, j], crecv.at[h, slot], c_s.at[h, slot], c_r.at[h, slot], peer_c))

    def wait_c(h, d, e, f):
        slot = (d * s + e) * zs + f
        remote(part.at[h, 0], crecv.at[h, slot], c_s.at[h, slot], c_r.at[h, slot], peer_c).wait_recv()

    def pair(h, d, e, f):
        j = dev(core, (a + d) % s, (b + e) % s, (z + f) % zs)
        return part[h, j] + crecv[h, (d * s + e) * zs + f]

    e_order = list(range(1, s)) + [0]
    f_order = [f for f in (2, 1, 3) if f < zs] + [0]

    def copy_a(h, d, e, f):
        at = ((d - 1) * s + e) * zs + f
        return remote(asend.at[h, at], arecv.at[h, at], a_s.at[h, at], a_r.at[h, at], peer_a[d])

    def copy_b(h, e, f):
        at = (e - 1) * zs + f
        return remote(bsend.at[h, at], brecv.at[h, at], b_s.at[h, at], b_r.at[h, at], peer_b[e])

    def copy_z(h, f):
        return remote(zsend.at[h, f - 1], zrecv.at[h, f - 1], z_s.at[h, f - 1], z_r.at[h, f - 1], peer_z[f])

    def stage_a(h):
        for e in e_order:
            for f in f_order:
                for d in range(1, s):
                    wait_c(h, d, e, f)
                    asend[h, ((d - 1) * s + e) * zs + f] = pair(h, d, e, f).astype(BF16)
                    go(copy_a(h, d, e, f))

    def after_a(h, e, f):
        wait_c(h, 0, e, f)
        total = pair(h, 0, e, f)
        for d in range(1, s):
            copy_a(h, d, e, f).wait_recv()
            total += arecv[h, ((d - 1) * s + e) * zs + f].astype(F32)
        return total

    def stage_b(h):
        for f in f_order:
            for e in range(1, s):
                bsend[h, (e - 1) * zs + f] = after_a(h, e, f)
                go(copy_b(h, e, f))

    def after_b(h, f):
        total = after_a(h, 0, f)
        for e in range(1, s):
            copy_b(h, e, f).wait_recv()
            total += brecv[h, (e - 1) * zs + f]
        return total

    def stage_z(h):
        for f in f_order[:-1]:
            zsend[h, f - 1] = after_b(h, f).astype(BF16)
            go(copy_z(h, f))

    def finish(h):
        total = after_b(h, 0)
        for f in range(1, zs):
            copy_z(h, f).wait_recv()
            total += zrecv[h, f - 1].astype(F32)
        return total

    def store(h, i, product):
        turned = product.T
        for k in range(per):
            part[h, i * per + k] = turned[k * rows : (k + 1) * rows]

    head = ht_ref[...].T
    for i in range(steps):
        oc_in[i].wait()
        store(0, i, jnp.dot(head, oc[:, i * chunk : (i + 1) * chunk], preferred_element_type=F32))
        send_chunk(0, i)

    group = 16
    for i in range(4):
        hid_in[i].wait()

        @pl.loop(0, hrow // group)
        def squares(t, i=i):
            at = pl.multiple_of(i * hrow + t * group, group)
            wide = hid[pl.ds(at, group)].astype(F32)
            inv[pl.ds(at, group)] = lax.rsqrt(jnp.sum(wide * wide, axis=1, keepdims=True) / width + norm_eps)

    stage_a(0)

    scaled = qt_ref[...].astype(F32) * inv[...]
    high = scaled.astype(BF16)
    low = (scaled - high.astype(F32)).astype(BF16)
    both = jnp.concatenate([high, low], axis=1).T
    cols = qt_ref.shape[1]
    for i in range(steps):
        product = jnp.dot(both, hid[:, i * chunk : (i + 1) * chunk], preferred_element_type=F32)
        store(1, i, (product[:cols] + product[cols:]) * gain_ref[:, i * chunk : (i + 1) * chunk])
        send_chunk(1, i)

    stage_b(0)
    stage_a(1)
    stage_z(0)
    stage_b(1)
    stage_z(1)
    grad_o = finish(0)
    part[0, me] = grad_o
    grad_q = finish(1)
    part[1, me] = grad_q

    square = jnp.sum(grad_q * grad_q) + jnp.sum(grad_o * grad_o)
    value = jnp.full(sbuf.shape[1:], square, F32)
    at_sem = 0
    for buf, place, size, to in ((sbuf, spot, plane, peer_p), (tbuf, z, zs, peer_z)):
        buf[place] = value
        copies = []
        for d in range(1, size):
            copy = remote(buf.at[place], buf.at[place], s_s.at[at_sem], s_r.at[at_sem], to[d])
            at_sem += 1
            go(copy)
            copies.append(copy)
        for copy in copies:
            copy.wait_recv()
        value = buf[0]
        for k in range(1, size):
            value = value + buf[k]
    rms = jnp.sqrt(value / (2.0 * width * cols))
    rms_ref[...] = rms
    factor = jnp.minimum(1.0, clip_rms / rms)[:1]

    def shard(h, d, e, f):
        return gbuf[h].at[dev(core, (a - d + s) % s, (b - e + s) % s, (z - f + zs) % zs)]

    def gather_z(h, f):
        return remote(shard(h, 0, 0, 0), shard(h, 0, 0, 0), gz_s.at[h, f - 1], gz_r.at[h, f - 1], peer_z[f])

    def gather_b(h, e, f):
        at = (e - 1) * zs + f
        return remote(shard(h, 0, 0, f), shard(h, 0, 0, f), gb_s.at[h, at], gb_r.at[h, at], peer_b[e])

    def gather_a(h, d, e, f):
        at = ((d - 1) * s + e) * zs + f
        return remote(shard(h, 0, e, f), shard(h, 0, e, f), ga_s.at[h, at], ga_r.at[h, at], peer_a[d])

    def gather_c(h, d, e, f):
        at = (d * s + e) * zs + f
        return remote(shard(h, d, e, f), shard(h, d, e, f), gc_s.at[h, at], gc_r.at[h, at], peer_c)

    def pass_a(h, e, f):
        for d in range(1, s):
            go(gather_a(h, d, e, f))
        go(gather_c(h, 0, e, f))

    def pass_b(h, f):
        if f:
            gather_z(h, f).wait_recv()
        for e in range(1, s):
            go(gather_b(h, e, f))
        pass_a(h, 0, f)

    def from_b(h, f):
        for e in range(1, s):
            gather_b(h, e, f).wait_recv()
            pass_a(h, e, f)

    def from_a(h, f):
        for e in range(s):
            for d in range(1, s):
                gather_a(h, d, e, f).wait_recv()
                go(gather_c(h, d, e, f))

    for copy in states:
        copy.wait()
    for h in range(2):
        master, moment, second = adamw(st_ref[3 * h], st_ref[3 * h + 1], st_ref[3 * h + 2], part[h, me], factor)
        gbuf[h][me] = master.astype(BF16)
        for f in range(1, zs):
            go(gather_z(h, f))
        pass_b(h, 0)
        new_ref[3 * h] = master
        new_ref[3 * h + 1] = moment
        new_ref[3 * h + 2] = second

    order = [0] + [f for f in (1, 3, 2) if f < zs]
    for t, f in enumerate(order):
        for h in range(2):
            if f:
                pass_b(h, f)
        for h in range(2):
            from_b(h, f)
        for h in range(2):
            if t:
                from_a(h, order[t - 1])
    for h in range(2):
        from_a(h, order[-1])
    for h in range(2):
        for d in range(s):
            for e in range(s):
                for f in range(zs):
                    gather_c(h, d, e, f).wait_recv()
    for copy in sends:
        copy.wait_send()


def shards(
    hidden, norm_gain, q_cotangent, head_output, out_cotangent,
    master_q, moment_q, second_q, master_o, moment_o, second_o,
    *, n,
):
    tokens, width = hidden.shape
    rows, cols = master_q.shape
    zs = 4
    s = math.isqrt(n // (2 * zs))
    slots = s * s * zs
    state = (master_o.T, moment_o.T, second_o.T, master_q, moment_q, second_q)
    any_spec = pl.BlockSpec(memory_space=pl.ANY)
    vmem = pl.BlockSpec(memory_space=pltpu.VMEM)
    dma = pltpu.SemaphoreType.DMA
    na, nb, nz = (s - 1) * s * zs, (s - 1) * zs, zs - 1
    tile = (rows, cols)
    gathered_o, gathered_q, new, rms = pl.pallas_call(
        functools.partial(kernel, n, s, zs),
        out_shape=(
            jax.ShapeDtypeStruct((n,) + tile, BF16),
            jax.ShapeDtypeStruct((n,) + tile, BF16),
            jax.ShapeDtypeStruct((6,) + tile, F32),
            jax.ShapeDtypeStruct((8, 128), F32),
        ),
        in_specs=[any_spec, vmem, vmem, vmem, any_spec] + [any_spec] * 6,
        out_specs=(vmem, vmem, vmem, vmem),
        scratch_shapes=[
            pltpu.VMEM((6,) + tile, F32),
            pltpu.VMEM((tokens, width), BF16),
            pltpu.VMEM((tokens, width), BF16),
            pltpu.VMEM((tokens, 1), F32),
            pltpu.VMEM((2, n) + tile, F32),
            pltpu.VMEM((2, slots) + tile, F32),
            pltpu.VMEM((2, na) + tile, BF16),
            pltpu.VMEM((2, na) + tile, BF16),
            pltpu.VMEM((2, nb) + tile, F32),
            pltpu.VMEM((2, nb) + tile, F32),
            pltpu.VMEM((2, nz) + tile, BF16),
            pltpu.VMEM((2, nz) + tile, BF16),
            pltpu.VMEM((2 * s * s, 8, 128), F32),
            pltpu.VMEM((zs, 8, 128), F32),
            dma((6,)), dma((4,)), dma((64,)),
            dma((2, slots)), dma((2, slots)),
            dma((2, na)), dma((2, na)),
            dma((2, nb)), dma((2, nb)),
            dma((2, nz)), dma((2, nz)),
            dma((2 * s * s + zs,)), dma((2 * s * s + zs,)),
            dma((2, nz)), dma((2, nz)),
            dma((2, nb)), dma((2, nb)),
            dma((2, na)), dma((2, na)),
            dma((2, slots)), dma((2, slots)),
        ],
        compiler_params=pltpu.CompilerParams(
            collective_id=0, has_side_effects=True, vmem_limit_bytes=60 * 1024 * 1024
        ),
    )(hidden, norm_gain[None, :], q_cotangent, head_output, out_cotangent, *state)
    q_param = gathered_q.reshape(width, cols)
    o_param = gathered_o.reshape(width, cols).T
    return (
        q_param, o_param,
        new[3], new[4], new[5],
        new[0].T, new[1].T, new[2].T,
        rms[0, 0],
    )


def solution(mesh):
    row, col = P("dp", None), P(None, "dp")
    in_specs = (row, P(), row, row, row, row, row, row, col, col, col)
    out_specs = (P(), P(), row, row, row, col, col, col, P())
    body = functools.partial(shards, n=mesh.shape["dp"])
    return jax.shard_map(body, mesh=mesh, in_specs=in_specs, out_specs=out_specs, check_vma=False)
```
